32 devices in a mesh: dp: 4 (over x, y), cp: 8 (over z, core).
Axes of the slice: x: 2, y: 2, z: 4, core: 2. Of those that a mesh axis runs over, the one named last changes fastest.
Arguments:
- images: bfloat16 [128, 256, 768], P('dp', 'cp'), parts along dimension 0
- ln1_scale: float32 [768], replicated
- ln1_bias: float32 [768], replicated
- w_qkv: bfloat16 [768, 3, 12, 64], replicated
- b_qkv: float32 [3, 12, 64], replicated
- w_out: bfloat16 [12, 64, 768], replicated
- b_out: float32 [768], replicated
- ln2_scale: float32 [768], replicated
- ln2_bias: float32 [768], replicated
- w_up: bfloat16 [768, 3072], replicated
- b_up: float32 [3072], replicated
- w_down: bfloat16 [3072, 768], replicated
- b_down: float32 [768], replicated
- lnf_scale: float32 [768], replicated
- lnf_bias: float32 [768], replicated
- pool_probe: bfloat16 [1, 768], replicated
- pool_wq: bfloat16 [768, 12, 64], replicated
- pool_bq: float32 [12, 64], replicated
- pool_wkv: bfloat16 [768, 2, 12, 64], replicated
- pool_bkv: float32 [2, 12, 64], replicated
- pool_wout: bfloat16 [12, 64, 768], replicated
- pool_bout: float32 [768], replicated
- pool_ln_scale: float32 [768], replicated
- pool_ln_bias: float32 [768], replicated
- pool_w_up: bfloat16 [768, 3072], replicated
- pool_b_up: float32 [3072], replicated
- pool_w_down: bfloat16 [3072, 768], replicated
- pool_b_down: float32 [768], replicated
Outputs:
- output: float32 [128, 768], P('dp'), parts along dimension 0
There are 4 independent parts. The reference program is written for one: setup_inputs(seed, part) draws one part's arguments, and reference() takes and returns one part's arrays. A program takes and returns all parts, laid end to end along the dimension named above; an argument that names none is the same for every part.
All inputs are finite; a program needn't handle non-finite values.
Results may differ from the reference program's by a relative error of at most 0.00999552.
Values are sent between devices in bfloat16 or wider.
A program may use at most 1 GiB of HBM per device.

```python
import math
import jax
import jax.numpy as jnp
from jax import lax

IMAGES = 32
TOKENS = 256
MODEL_DIM = 768
NUM_HEADS = 12
HEAD_DIM = 64
MLP_DIM = 3072

ROW_BLOCK = TOKENS // 16
GRID_SIDE = math.isqrt(TOKENS)


def weight_draw(rand_key, arr_shape, fan_in):
    return (jax.random.normal(rand_key, arr_shape, jnp.float32) * fan_in ** -0.5).astype(jnp.bfloat16)


def gain_draw(rand_key, arr_shape):
    return 1.0 + 0.2 * jax.random.normal(rand_key, arr_shape, jnp.float32)


def shift_draw(rand_key, arr_shape):
    return 0.2 * jax.random.normal(rand_key, arr_shape, jnp.float32)


def setup_inputs(seed: int = 0, part: int = 0) -> dict:
    root_key = jax.random.key(seed)
    halves = jax.random.split(root_key, 2)
    image_keys = jax.random.split(jax.random.fold_in(halves[0], part), 5)
    weight_keys = jax.random.split(halves[1], 27)
    wave_count = 8
    positions = jnp.arange(TOKENS)
    grid_rows = (positions // GRID_SIDE).astype(jnp.float32) / GRID_SIDE
    grid_cols = (positions % GRID_SIDE).astype(jnp.float32) / GRID_SIDE
    freq_rows = jax.random.randint(image_keys[0], (IMAGES, wave_count), 1, 4).astype(jnp.float32)
    freq_cols = jax.random.randint(image_keys[1], (IMAGES, wave_count), 0, 4).astype(jnp.float32)
    phases = jax.random.uniform(image_keys[2], (IMAGES, wave_count), jnp.float32, 0.0, 2.0 * math.pi)
    wave_rows = jnp.cos(2.0 * math.pi * (freq_rows[:, :, None] * grid_rows + freq_cols[:, :, None] * grid_cols) + phases[:, :, None])
    directions = jax.random.normal(image_keys[3], (IMAGES, wave_count, MODEL_DIM), jnp.float32) * (2.0 / wave_count) ** 0.5
    wave_field = jnp.einsum("bwn,bwd->bnd", wave_rows, directions)
    noise_part = jax.random.normal(image_keys[4], (IMAGES, TOKENS, MODEL_DIM), jnp.float32)
    return {
        "images": (wave_field + 0.5 * noise_part).astype(jnp.bfloat16),
        "ln1_scale": gain_draw(weight_keys[0], (MODEL_DIM,)),
        "ln1_bias": shift_draw(weight_keys[1], (MODEL_DIM,)),
        "w_qkv": weight_draw(weight_keys[2], (MODEL_DIM, 3, NUM_HEADS, HEAD_DIM), MODEL_DIM),
        "b_qkv": shift_draw(weight_keys[3], (3, NUM_HEADS, HEAD_DIM)),
        "w_out": weight_draw(weight_keys[4], (NUM_HEADS, HEAD_DIM, MODEL_DIM), MODEL_DIM),
        "b_out": shift_draw(weight_keys[5], (MODEL_DIM,)),
        "ln2_scale": gain_draw(weight_keys[6], (MODEL_DIM,)),
        "ln2_bias": shift_draw(weight_keys[7], (MODEL_DIM,)),
        "w_up": weight_draw(weight_keys[8], (MODEL_DIM, MLP_DIM), MODEL_DIM),
        "b_up": shift_draw(weight_keys[9], (MLP_DIM,)),
        "w_down": weight_draw(weight_keys[10], (MLP_DIM, MODEL_DIM), MLP_DIM),
        "b_down": shift_draw(weight_keys[11], (MODEL_DIM,)),
        "lnf_scale": gain_draw(weight_keys[12], (MODEL_DIM,)),
        "lnf_bias": shift_draw(weight_keys[13], (MODEL_DIM,)),
        "pool_probe": jax.random.normal(weight_keys[14], (1, MODEL_DIM), jnp.float32).astype(jnp.bfloat16),
        "pool_wq": weight_draw(weight_keys[15], (MODEL_DIM, NUM_HEADS, HEAD_DIM), MODEL_DIM),
        "pool_bq": shift_draw(weight_keys[16], (NUM_HEADS, HEAD_DIM)),
        "pool_wkv": weight_draw(weight_keys[17], (MODEL_DIM, 2, NUM_HEADS, HEAD_DIM), MODEL_DIM),
        "pool_bkv": shift_draw(weight_keys[18], (2, NUM_HEADS, HEAD_DIM)),
        "pool_wout": weight_draw(weight_keys[19], (NUM_HEADS, HEAD_DIM, MODEL_DIM), MODEL_DIM),
        "pool_bout": shift_draw(weight_keys[20], (MODEL_DIM,)),
        "pool_ln_scale": gain_draw(weight_keys[21], (MODEL_DIM,)),
        "pool_ln_bias": shift_draw(weight_keys[22], (MODEL_DIM,)),
        "pool_w_up": weight_draw(weight_keys[23], (MODEL_DIM, MLP_DIM), MODEL_DIM),
        "pool_b_up": shift_draw(weight_keys[24], (MLP_DIM,)),
        "pool_w_down": weight_draw(weight_keys[25], (MLP_DIM, MODEL_DIM), MLP_DIM),
        "pool_b_down": shift_draw(weight_keys[26], (MODEL_DIM,)),
    }


def layer_norm(values, ln_gain, ln_shift):
    row_mean = jnp.mean(values, axis=-1, keepdims=True)
    centered = values - row_mean
    variance = jnp.mean(centered * centered, axis=-1, keepdims=True)
    return centered * lax.rsqrt(variance + 1e-6) * ln_gain + ln_shift


def reference(images, ln1_scale, ln1_bias, w_qkv, b_qkv, w_out, b_out, ln2_scale, ln2_bias, w_up, b_up, w_down, b_down, lnf_scale, lnf_bias, pool_probe, pool_wq, pool_bq, pool_wkv, pool_bkv, pool_wout, pool_bout, pool_ln_scale, pool_ln_bias, pool_w_up, pool_b_up, pool_w_down, pool_b_down):
    score_scale = HEAD_DIM ** -0.5
    probe_q = (jnp.einsum("od,dhe->he", pool_probe.astype(jnp.float32), pool_wq.astype(jnp.float32)) + pool_bq).astype(jnp.bfloat16)

    def one_image(image_tokens):
        resid_in = image_tokens.astype(jnp.float32)
        normed = layer_norm(resid_in, ln1_scale, ln1_bias).astype(jnp.bfloat16)
        qkv = (jnp.einsum("nd,dshe->snhe", normed.astype(jnp.float32), w_qkv.astype(jnp.float32)) + b_qkv[:, None]).astype(jnp.bfloat16)
        key_rows = qkv[1].astype(jnp.float32)
        value_rows = qkv[2].astype(jnp.float32)

        def attend_rows(query_rows):
            scores = jnp.einsum("qhe,khe->hqk", query_rows.astype(jnp.float32), key_rows) * score_scale
            weights = jnp.exp(scores - jnp.max(scores, axis=-1, keepdims=True))
            value_sum = jnp.einsum("hqk,khe->hqe", weights.astype(jnp.bfloat16).astype(jnp.float32), value_rows)
            return value_sum / jnp.sum(weights, axis=-1)[:, :, None]

        blocks = lax.map(attend_rows, qkv[0].reshape(TOKENS // ROW_BLOCK, ROW_BLOCK, NUM_HEADS, HEAD_DIM))
        context = blocks.transpose(1, 0, 2, 3).reshape(NUM_HEADS, TOKENS, HEAD_DIM).astype(jnp.bfloat16)
        attn_out = jnp.einsum("hne,hed->nd", context.astype(jnp.float32), w_out.astype(jnp.float32)) + b_out
        resid_mid = (resid_in + attn_out).astype(jnp.bfloat16)
        normed_mid = layer_norm(resid_mid.astype(jnp.float32), ln2_scale, ln2_bias).astype(jnp.bfloat16)
        hidden = jax.nn.gelu(jnp.dot(normed_mid, w_up, preferred_element_type=jnp.float32) + b_up, approximate=True).astype(jnp.bfloat16)
        layer_out = (resid_mid.astype(jnp.float32) + jnp.dot(hidden, w_down, preferred_element_type=jnp.float32) + b_down).astype(jnp.bfloat16)
        tokens_out = layer_norm(layer_out.astype(jnp.float32), lnf_scale, lnf_bias).astype(jnp.bfloat16)
        pool_kv = (jnp.einsum("nd,dshe->snhe", tokens_out.astype(jnp.float32), pool_wkv.astype(jnp.float32)) + pool_bkv[:, None]).astype(jnp.bfloat16)
        pool_scores = jnp.einsum("he,nhe->hn", probe_q.astype(jnp.float32), pool_kv[0].astype(jnp.float32)) * score_scale
        pool_weights = jnp.exp(pool_scores - jnp.max(pool_scores, axis=-1, keepdims=True))
        pool_sum = jnp.einsum("hn,nhe->he", pool_weights.astype(jnp.bfloat16).astype(jnp.float32), pool_kv[1].astype(jnp.float32))
        pooled = (pool_sum / jnp.sum(pool_weights, axis=-1)[:, None]).astype(jnp.bfloat16)
        pooled_out = (jnp.einsum("he,hed->d", pooled.astype(jnp.float32), pool_wout.astype(jnp.float32)) + pool_bout).astype(jnp.bfloat16)
        normed_out = layer_norm(pooled_out.astype(jnp.float32), pool_ln_scale, pool_ln_bias).astype(jnp.bfloat16)
        hidden_out = jax.nn.gelu(jnp.dot(normed_out[None], pool_w_up, preferred_element_type=jnp.float32)[0] + pool_b_up, approximate=True).astype(jnp.bfloat16)
        return pooled_out.astype(jnp.float32) + jnp.dot(hidden_out[None], pool_w_down, preferred_element_type=jnp.float32)[0] + pool_b_down

    return lax.map(one_image, images)
```

```python
import functools
import math

import jax
import jax.numpy as jnp
from jax import lax
from jax.experimental import pallas as pl
from jax.experimental.pallas import tpu as pltpu
from jax.sharding import PartitionSpec as P

MESH = pl.DeviceIdType.MESH
F32 = jnp.float32
BF16 = jnp.bfloat16
EPSILON = 1e-6
DIM = 768
HEADS = 12
HEAD = 64
MLP = 3072
GELU_C = math.sqrt(2.0 / math.pi)
LOG2E = math.log2(math.e)


def dot(left, right):
    return jnp.dot(left, right, preferred_element_type=F32)


def dot_nt(left, right):
    return lax.dot_general(left, right, (((1,), (1,)), ((), ())), preferred_element_type=F32)


def gelu(x):
    half = 0.5 * x
    return half + half * jnp.tanh(x * (GELU_C + (GELU_C * 0.044715) * (x * x)))


def layer_norm(values, gain, shift):
    row_mean = jnp.sum(values, axis=-1, keepdims=True) * (1.0 / DIM)
    centered = values - row_mean
    variance = jnp.sum(centered * centered, axis=-1, keepdims=True) * (1.0 / DIM)
    return centered * lax.rsqrt(variance + EPSILON) * gain + shift


def column_bias(bias, out_ref, base):
    eye = lax.broadcasted_iota(jnp.int32, (HEAD, HEAD), 0) == lax.broadcasted_iota(jnp.int32, (HEAD, HEAD), 1)
    for head in range(HEADS):
        spread = jnp.where(eye, jnp.broadcast_to(bias[head : head + 1, :], (HEAD, HEAD)), 0.0)
        column = jnp.sum(spread, axis=1, keepdims=True)
        out_ref[pl.ds(base + head * HEAD, HEAD), :] = jnp.broadcast_to(column, (HEAD, 128))


def row_bias(column_ref, base):
    eye = lax.broadcasted_iota(jnp.int32, (128, 128), 0) == lax.broadcasted_iota(jnp.int32, (128, 128), 1)
    parts = []
    for block in range(DIM // 128):
        tile = column_ref[pl.ds(base + block * 128, 128), :]
        parts.append(jnp.sum(jnp.where(eye, tile, 0.0), axis=0, keepdims=True))
    return jnp.concatenate(parts, axis=1)


def add_column(values, column):
    return values + jnp.concatenate([column, column], axis=1)


def kernel(
    group, local, run,
    images, ln1_g, ln1_c, w_qkv, b_qkv, w_out, b_out, ln2_g, ln2_c, w_up, b_up, w_down, b_down, lnf_g, lnf_c,
    probe, p_wq, p_bq, p_wkv, p_bkv, p_wout, p_bout, pln_g, pln_c, p_wup, p_bup, p_wdown, p_bdown,
    out_ref,
    x_buf, v_ln1_g, v_ln1_c, v_wqkv, v_bqkv, v_wout, v_bout, v_ln2_g, v_ln2_c, v_wup, v_bup, v_wdown, v_bdown, v_lnf_g, v_lnf_c,
    v_probe, v_pwq, v_pbq, v_pwkv, v_pbkv, v_pwout, v_pbout, v_plng, v_plnc, v_pwup, v_pbup, v_pwdown, v_pbdown,
    wk_t, col_qkv, col_q, col_kv, row_k, u_diag, h_buf, h_t, q_t, v_t, k_buf, c_t, r_buf, n_buf, m_buf, z_buf, kv_t, a_buf, emb,
    load_sem, own_sem, send_sem, recv_sem, emb_send, emb_recv,
):
    tokens = group * run
    me = lax.axis_index("cp")
    barrier = pltpu.get_barrier_semaphore()
    for k in range(1, group):
        pl.semaphore_signal(barrier, inc=1, device_id={"cp": me ^ k}, device_id_type=MESH)

    pairs = [
        (w_qkv, v_wqkv), (ln1_g, v_ln1_g), (ln1_c, v_ln1_c), (b_qkv, v_bqkv), (w_out, v_wout), (b_out, v_bout),
        (ln2_g, v_ln2_g), (ln2_c, v_ln2_c), (w_up, v_wup), (b_up, v_bup), (w_down, v_wdown), (b_down, v_bdown),
        (lnf_g, v_lnf_g), (lnf_c, v_lnf_c), (probe, v_probe), (p_wq, v_pwq), (p_bq, v_pbq), (p_wkv, v_pwkv),
        (p_bkv, v_pbkv), (p_wout, v_pwout), (p_bout, v_pbout), (pln_g, v_plng), (pln_c, v_plnc), (p_wup, v_pwup),
        (p_bup, v_pbup), (p_wdown, v_pwdown), (p_bdown, v_pbdown),
    ]
    loads = [pltpu.make_async_copy(src, dst, load_sem.at[i]) for i, (src, dst) in enumerate(pairs)]
    own = [pltpu.make_async_copy(images.at[me * local + s], x_buf.at[s, me], own_sem.at[s]) for s in range(local)]
    for copy in loads[:4]:
        copy.start()
    for copy in own:
        copy.start()

    def send(s, k):
        peer = me ^ k
        return pltpu.make_async_remote_copy(
            src_ref=images.at[peer * local + s],
            dst_ref=x_buf.at[s, me],
            send_sem=send_sem.at[s, k],
            recv_sem=recv_sem.at[s, k],
            device_id={"cp": peer},
            device_id_type=MESH,
        )

    order = sorted(range(1, group), key=lambda k: -k)
    pl.semaphore_wait(barrier, group - 1)
    for s in range(local):
        for k in order:
            send(s, k).start()
    for copy in loads[4:]:
        copy.start()
    for copy in loads[:4]:
        copy.wait()

    for part in range(3):
        column_bias(v_bqkv[part], col_qkv, part * DIM)
    row_k[...] = row_bias(col_qkv, DIM)
    for block in range(DIM // 256):
        wk_t[:, pl.ds(block * 256, 256)] = v_wqkv[pl.ds(DIM + block * 256, 256), :].T
    for copy in loads[4:]:
        copy.wait()
    column_bias(v_pbq[...], col_q, 0)
    column_bias(v_pbkv[:, 0, :], col_kv, 0)
    column_bias(v_pbkv[:, 1, :], col_kv, DIM)
    probe_rows = jnp.broadcast_to(v_probe[...].astype(F32), (16, DIM)).astype(BF16)
    probe_q = dot_nt(probe_rows, v_pwq[...]) + row_bias(col_q, 0)
    head_of_lane = lax.broadcasted_iota(jnp.int32, (16, DIM), 1) // HEAD
    diagonal = head_of_lane == lax.broadcasted_iota(jnp.int32, (16, DIM), 0)
    u_diag[...] = jnp.where(diagonal, probe_q, 0.0).astype(BF16)

    rows = 32
    a_buf[...] = jnp.zeros_like(a_buf)

    def one_image(s, _):
        pltpu.make_async_copy(images.at[0], x_buf.at[s, me], own_sem.at[s]).wait()
        for k in order:
            send(s, k).wait_recv()

        for piece in range(group):
            x = x_buf[s, piece].astype(F32)
            h_buf[pl.ds(piece * run, run), :] = layer_norm(x, v_ln1_g[...], v_ln1_c[...]).astype(BF16)
        h_t[...] = h_buf[...].T
        q_t[...] = add_column(dot(v_wqkv[pl.ds(0, DIM), :], h_t[...]), col_qkv[pl.ds(0, DIM), :]).astype(BF16)
        v_t[...] = add_column(dot(v_wqkv[pl.ds(2 * DIM, DIM), :], h_t[...]), col_qkv[pl.ds(2 * DIM, DIM), :]).astype(BF16)
        k_buf[...] = (dot(h_buf[...], wk_t[...]) + row_k[...]).astype(BF16)

        zero = jnp.zeros((HEAD, tokens), BF16)
        for pair in range(HEADS // 2):
            k_pair = k_buf[:, pl.ds(pair * 2 * HEAD, 2 * HEAD)]
            for side in range(2):
                head = 2 * pair + side
                q_head = q_t[pl.ds(head * HEAD, HEAD), :]
                q_pair = jnp.concatenate([q_head, zero] if side == 0 else [zero, q_head], axis=0)
                scores = dot(k_pair, q_pair)
                top = jnp.max(scores, axis=0, keepdims=True)
                weights = jnp.exp2((scores - top) * (LOG2E * HEAD**-0.5))
                total = jnp.sum(weights, axis=0, keepdims=True)
                value = dot(v_t[pl.ds(head * HEAD, HEAD), :], weights.astype(BF16))
                c_t[pl.ds(head * HEAD, HEAD), :] = (value / total).astype(BF16)

        h_buf[...] = c_t[...].T
        for block in range(DIM // 256):
            cols = pl.ds(block * 256, 256)
            attn = dot(h_buf[...], v_wout[:, cols]) + v_bout[:, cols]
            for piece in range(group):
                here = slice(piece * run, (piece + 1) * run)
                r_buf[here, cols] = (x_buf[s, piece, :, cols].astype(F32) + attn[here, :]).astype(BF16)
        for start in range(0, tokens, rows):
            here = pl.ds(start, rows)
            n_buf[here, :] = layer_norm(r_buf[here, :].astype(F32), v_ln2_g[...], v_ln2_c[...]).astype(BF16)
        for block in range(MLP // 256):
            cols = pl.ds(block * 256, 256)
            m_buf[:, cols] = gelu(dot(n_buf[...], v_wup[:, cols]) + v_bup[:, cols]).astype(BF16)
        for block in range(DIM // 256):
            cols = pl.ds(block * 256, 256)
            down = dot(m_buf[...], v_wdown[:, cols])
            h_buf[:, cols] = (r_buf[:, cols].astype(F32) + down + v_bdown[:, cols]).astype(BF16)
        for start in range(0, tokens, rows):
            here = pl.ds(start, rows)
            z_buf[here, :] = layer_norm(h_buf[here, :].astype(F32), v_lnf_g[...], v_lnf_c[...]).astype(BF16)
        h_t[...] = z_buf[...].T
        for part in range(2):
            here = pl.ds(part * DIM, DIM)
            kv_t[here, :] = add_column(dot(v_pwkv[here, :], h_t[...]), col_kv[here, :]).astype(BF16)
        scores = dot(u_diag[...], kv_t[pl.ds(0, DIM), :])
        top = jnp.max(scores, axis=1, keepdims=True)
        weights = jnp.exp2((scores - top) * (LOG2E * HEAD**-0.5))
        total = jnp.sum(weights, axis=1, keepdims=True)
        value = dot_nt(weights.astype(BF16), kv_t[pl.ds(DIM, DIM), :]) / total
        pooled = jnp.sum(jnp.where(diagonal, value, 0.0), axis=0, keepdims=True)
        a_buf[...] = jnp.where(lax.broadcasted_iota(jnp.int32, (8, DIM), 0) == s, pooled, a_buf[...])
        return 0

    lax.fori_loop(0, local, one_image, 0)

    pooled = a_buf[...].astype(BF16)
    o = (dot(pooled, v_pwout[...]) + v_pbout[...]).astype(BF16)
    normed = layer_norm(o.astype(F32), v_plng[...], v_plnc[...]).astype(BF16)
    hidden = gelu(dot(normed, v_pwup[...]) + v_pbup[...]).astype(BF16)
    emb[...] = (o.astype(F32) + dot(hidden, v_pwdown[...]) + v_pbdown[...])[:local, :]

    def share(k):
        return pltpu.make_async_remote_copy(
            src_ref=emb,
            dst_ref=out_ref.at[me],
            send_sem=emb_send.at[k],
            recv_sem=emb_recv.at[k],
            device_id={"cp": me ^ k},
            device_id_type=MESH,
        )

    for k in order:
        share(k).start()
    out_ref[me] = emb[...]
    for s in range(local):
        for k in order:
            send(s, k).wait_send()
    for k in order:
        share(k).wait()


def solution(mesh):
    group = mesh.shape["cp"]

    def device_step(
        images, ln1_scale, ln1_bias, w_qkv, b_qkv, w_out, b_out, ln2_scale, ln2_bias, w_up, b_up, w_down, b_down, lnf_scale, lnf_bias,
        pool_probe, pool_wq, pool_bq, pool_wkv, pool_bkv, pool_wout, pool_bout, pool_ln_scale, pool_ln_bias, pool_w_up, pool_b_up,
        pool_w_down, pool_b_down,
    ):
        count, run, _ = images.shape
        local = count // group
        tokens = group * run

        def row(vector):
            return vector.reshape(1, -1)

        operands = [
            images, row(ln1_scale), row(ln1_bias), w_qkv.transpose(1, 2, 3, 0).reshape(3 * DIM, DIM), b_qkv,
            w_out.reshape(DIM, DIM), row(b_out), row(ln2_scale), row(ln2_bias), w_up, row(b_up), w_down, row(b_down),
            row(lnf_scale), row(lnf_bias), pool_probe, pool_wq.transpose(1, 2, 0).reshape(DIM, DIM), pool_bq,
            pool_wkv.transpose(1, 2, 3, 0).reshape(2 * DIM, DIM), pool_bkv.transpose(1, 0, 2), pool_wout.reshape(DIM, DIM),
            row(pool_bout), row(pool_ln_scale), row(pool_ln_bias), pool_w_up, row(pool_b_up), pool_w_down, row(pool_b_down),
        ]
        held = [pltpu.VMEM(operand.shape, operand.dtype) for operand in operands[1:]]
        scratch = [
            pltpu.VMEM((local, group, run, DIM), BF16),
            *held,
            pltpu.VMEM((DIM, DIM), BF16),
            pltpu.VMEM((3 * DIM, 128), F32),
            pltpu.VMEM((DIM, 128), F32),
            pltpu.VMEM((2 * DIM, 128), F32),
            pltpu.VMEM((1, DIM), F32),
            pltpu.VMEM((16, DIM), BF16),
            pltpu.VMEM((tokens, DIM), BF16),
            pltpu.VMEM((DIM, tokens), BF16),
            pltpu.VMEM((DIM, tokens), BF16),
            pltpu.VMEM((DIM, tokens), BF16),
            pltpu.VMEM((tokens, DIM), BF16),
            pltpu.VMEM((DIM, tokens), BF16),
            pltpu.VMEM((tokens, DIM), BF16),
            pltpu.VMEM((tokens, DIM), BF16),
            pltpu.VMEM((tokens, MLP), BF16),
            pltpu.VMEM((tokens, DIM), BF16),
            pltpu.VMEM((2 * DIM, tokens), BF16),
            pltpu.VMEM((8, DIM), F32),
            pltpu.VMEM((local, DIM), F32),
            pltpu.SemaphoreType.DMA((len(held),)),
            pltpu.SemaphoreType.DMA((local,)),
            pltpu.SemaphoreType.DMA((local, group)),
            pltpu.SemaphoreType.DMA((local, group)),
            pltpu.SemaphoreType.DMA((group,)),
            pltpu.SemaphoreType.DMA((group,)),
        ]
        result = pl.pallas_call(
            functools.partial(kernel, group, local, run),
            out_shape=jax.ShapeDtypeStruct((group, local, DIM), F32),
            in_specs=[pl.BlockSpec(memory_space=pl.ANY)] * len(operands),
            out_specs=pl.BlockSpec(memory_space=pltpu.VMEM),
            scratch_shapes=scratch,
            compiler_params=pltpu.CompilerParams(collective_id=0, has_side_effects=True, vmem_limit_bytes=67_043_328),
        )(*operands)
        return result.reshape(count, DIM)

    in_specs = (P("dp", "cp", None),) + (P(),) * 27
    return jax.shard_map(device_step, mesh=mesh, in_specs=in_specs, out_specs=P("dp", None), check_vma=False)
```

```python
import functools
import math

import jax
import jax.numpy as jnp
from jax import lax
from jax.experimental import pallas as pl
from jax.experimental.pallas import tpu as pltpu
from jax.sharding import PartitionSpec as P

MESH = pl.DeviceIdType.MESH
F32 = jnp.float32
BF16 = jnp.bfloat16
EPSILON = 1e-6
DIM = 768
HEADS = 12
HEAD = 64
MLP = 3072
GELU_C = math.sqrt(2.0 / math.pi)
LOG2E = math.log2(math.e)


def dot(left, right):
    return jnp.dot(left, right, preferred_element_type=F32)


def dot_nt(left, right):
    return lax.dot_general(left, right, (((1,), (1,)), ((), ())), preferred_element_type=F32)


def as_row(ref, cols=slice(None)):
    return ref[cols][None, :]


def gelu(x):
    half = 0.5 * x
    return half + half * jnp.tanh(x * (GELU_C + (GELU_C * 0.044715) * (x * x)))


def layer_norm(values, gain, shift):
    row_mean = jnp.sum(values, axis=-1, keepdims=True) * (1.0 / DIM)
    centered = values - row_mean
    variance = jnp.sum(centered * centered, axis=-1, keepdims=True) * (1.0 / DIM)
    return centered * lax.rsqrt(variance + EPSILON) * gain + shift


def column_bias(bias, out_ref, base):
    eye = lax.broadcasted_iota(jnp.int32, (HEAD, HEAD), 0) == lax.broadcasted_iota(jnp.int32, (HEAD, HEAD), 1)
    for head in range(HEADS):
        spread = jnp.where(eye, jnp.broadcast_to(bias[head : head + 1, :], (HEAD, HEAD)), 0.0)
        column = jnp.sum(spread, axis=1, keepdims=True)
        out_ref[pl.ds(base + head * HEAD, HEAD), :] = jnp.broadcast_to(column, (HEAD, 128))


def row_bias(column_ref, base):
    eye = lax.broadcasted_iota(jnp.int32, (128, 128), 0) == lax.broadcasted_iota(jnp.int32, (128, 128), 1)
    parts = []
    for block in range(DIM // 128):
        tile = column_ref[pl.ds(base + block * 128, 128), :]
        parts.append(jnp.sum(jnp.where(eye, tile, 0.0), axis=0, keepdims=True))
    return jnp.concatenate(parts, axis=1)


def add_column(values, column):
    return values + jnp.concatenate([column, column], axis=1)


def kernel(
    group, local, run,
    images, ln1_g, ln1_c, w_qkv, b_qkv, w_out, b_out, ln2_g, ln2_c, w_up, b_up, w_down, b_down, lnf_g, lnf_c,
    probe, p_wq, p_bq, p_wkv, p_bkv, p_wout, p_bout, pln_g, pln_c, p_wup, p_bup, p_wdown, p_bdown,
    out_ref,
    x_buf, v_ln1_g, v_ln1_c, v_wqkv, v_bqkv, v_wout, v_bout, v_ln2_g, v_ln2_c, v_wup, v_bup, v_wdown, v_bdown, v_lnf_g, v_lnf_c,
    v_probe, v_pwq, v_pbq, v_pwkv, v_pbkv, v_pwout, v_pbout, v_plng, v_plnc, v_pwup, v_pbup, v_pwdown, v_pbdown,
    wk_t, col_qkv, col_q, col_kv, row_k, u_diag, h_buf, h_t, q_t, v_t, k_buf, c_t, r_buf, n_buf, m_buf, z_buf, kv_t, s_buf, w_buf, t_buf, a_buf, emb,
    load_sem, own_sem, send_sem, recv_sem, emb_send, emb_recv, relay,
):
    tokens = group * run
    me = lax.axis_index("cp")
    chip = me // 2
    inner = (chip == 1) | (chip == 2)

    def tell(semaphore, k):
        pl.semaphore_signal(semaphore, inc=1, device_id={"cp": me ^ k}, device_id_type=MESH)

    barrier = pltpu.get_barrier_semaphore()
    for k in (2, 3, 1):
        tell(barrier, k)

    @pl.when(inner)
    def _():
        tell(barrier, 6)
        tell(barrier, 7)

    pairs = [
        (w_qkv, v_wqkv), (ln1_g, v_ln1_g), (ln1_c, v_ln1_c), (b_qkv, v_bqkv), (w_out, v_wout), (b_out, v_bout),
        (ln2_g, v_ln2_g), (ln2_c, v_ln2_c), (w_up, v_wup), (b_up, v_bup), (w_down, v_wdown), (b_down, v_bdown),
        (lnf_g, v_lnf_g), (lnf_c, v_lnf_c), (probe, v_probe), (p_wq, v_pwq), (p_bq, v_pbq), (p_wkv, v_pwkv),
        (p_bkv, v_pbkv), (p_wout, v_pwout), (p_bout, v_pbout), (pln_g, v_plng), (pln_c, v_plnc), (p_wup, v_pwup),
        (p_bup, v_pbup), (p_wdown, v_pwdown), (p_bdown, v_pbdown),
    ]
    loads = [pltpu.make_async_copy(src, dst, load_sem.at[i]) for i, (src, dst) in enumerate(pairs)]
    own = [pltpu.make_async_copy(images.at[me * local + s], x_buf.at[s, me], own_sem.at[s]) for s in range(local)]
    for copy in loads[:4]:
        copy.start()
    for copy in own:
        copy.start()

    def send(s, k):
        peer = me ^ k
        return pltpu.make_async_remote_copy(
            src_ref=images.at[peer * local + s],
            dst_ref=x_buf.at[s, me],
            send_sem=send_sem.at[s, k],
            recv_sem=recv_sem.at[s, k],
            device_id={"cp": peer},
            device_id_type=MESH,
        )

    far, near = (6, 7, 4, 5), (2, 3, 1)
    order = far + near

    @pl.when(inner)
    def _():
        pl.semaphore_wait(barrier, 5)
        send(0, 6).start()
        send(0, 7).start()
        tell(relay.at[0], 2)
        tell(relay.at[0], 6)

    @pl.when(jnp.logical_not(inner))
    def _():
        pl.semaphore_wait(barrier, 3)

    for k in near:
        send(0, k).start()
    for copy in loads[4:]:
        copy.start()
    pl.semaphore_wait(relay.at[0], 1)

    @pl.when(inner)
    def _():
        tell(relay.at[1], 2)

    send(0, 4).start()
    send(0, 5).start()

    @pl.when(jnp.logical_not(inner))
    def _():
        pl.semaphore_wait(relay.at[1], 1)
        send(0, 6).start()
        send(0, 7).start()

    for copy in loads[:4]:
        copy.wait()

    for part in range(3):
        column_bias(v_bqkv[part], col_qkv, part * DIM)
    row_k[...] = row_bias(col_qkv, DIM)
    for block in range(DIM // 256):
        wk_t[:, pl.ds(block * 256, 256)] = v_wqkv[pl.ds(DIM + block * 256, 256), :].T
    for copy in loads[4:]:
        copy.wait()
    column_bias(v_pbq[...], col_q, 0)
    column_bias(v_pbkv[:, 0, :], col_kv, 0)
    column_bias(v_pbkv[:, 1, :], col_kv, DIM)
    probe_rows = jnp.broadcast_to(v_probe[...].astype(F32), (16, DIM)).astype(BF16)
    probe_q = dot_nt(probe_rows, v_pwq[...]) + row_bias(col_q, 0)
    head_of_lane = lax.broadcasted_iota(jnp.int32, (16, DIM), 1) // HEAD
    diagonal = head_of_lane == lax.broadcasted_iota(jnp.int32, (16, DIM), 0)
    u_diag[...] = jnp.where(diagonal, probe_q, 0.0).astype(BF16)

    rows = 32
    a_buf[...] = jnp.zeros_like(a_buf)
    for k in far:
        send(0, k).wait_send()
    for k in order:
        send(1, k).start()

    def one_image(s, _):
        pltpu.make_async_copy(images.at[0], x_buf.at[s, me], own_sem.at[s]).wait()
        for k in order:
            send(s, k).wait_recv()

        for piece in range(group):
            x = x_buf[s, piece].astype(F32)
            h_buf[pl.ds(piece * run, run), :] = layer_norm(x, as_row(v_ln1_g), as_row(v_ln1_c)).astype(BF16)
        h_t[...] = h_buf[...].T

        q_t[...] = add_column(dot(v_wqkv[pl.ds(0, DIM), :], h_t[...]), col_qkv[pl.ds(0, DIM), :]).astype(BF16)
        v_t[...] = add_column(dot(v_wqkv[pl.ds(2 * DIM, DIM), :], h_t[...]), col_qkv[pl.ds(2 * DIM, DIM), :]).astype(BF16)
        k_buf[...] = (dot(h_buf[...], wk_t[...]) + row_k[...]).astype(BF16)

        pairs = HEADS // 2
        zero = jnp.zeros((HEAD, tokens), BF16)
        for step in range(pairs + 2):
            if step < pairs:
                k_pair = k_buf[:, pl.ds(step * 2 * HEAD, 2 * HEAD)]
                low = q_t[pl.ds(2 * step * HEAD, HEAD), :]
                high = q_t[pl.ds((2 * step + 1) * HEAD, HEAD), :]
                s_buf[step % 2, :, pl.ds(0, tokens)] = dot(k_pair, jnp.concatenate([low, zero], axis=0))
                s_buf[step % 2, :, pl.ds(tokens, tokens)] = dot(k_pair, jnp.concatenate([zero, high], axis=0))
            if 1 <= step <= pairs:
                slot = (step - 1) % 2
                for block in range(2 * tokens // 128):
                    cols = pl.ds(block * 128, 128)
                    top = jnp.max(s_buf[slot, :, cols], axis=0, keepdims=True)
                    weights = jnp.exp2((s_buf[slot, :, cols] - top) * (LOG2E * HEAD**-0.5))
                    t_buf[slot, :, cols] = 1.0 / jnp.sum(weights, axis=0, keepdims=True)
                    w_buf[slot, :, cols] = weights.astype(BF16)
            if step >= 2:
                slot = step % 2
                for side in range(2):
                    here = pl.ds((2 * (step - 2) + side) * HEAD, HEAD)
                    cols = pl.ds(side * tokens, tokens)
                    c_t[here, :] = (dot(v_t[here, :], w_buf[slot, :, cols]) * t_buf[slot, :, cols]).astype(BF16)

        h_buf[...] = c_t[...].T

        attn = dot(h_buf[...], v_wout[...]) + as_row(v_bout)
        for piece in range(group):
            here = slice(piece * run, (piece + 1) * run)
            r_buf[here, :] = (x_buf[s, piece].astype(F32) + attn[here, :]).astype(BF16)
        for start in range(0, tokens, rows):
            here = pl.ds(start, rows)
            n_buf[here, :] = layer_norm(r_buf[here, :].astype(F32), as_row(v_ln2_g), as_row(v_ln2_c)).astype(BF16)

        for block in range(MLP // 512):
            cols = pl.ds(block * 512, 512)
            m_buf[:, cols] = gelu(dot(n_buf[...], v_wup[:, cols]) + as_row(v_bup, cols)).astype(BF16)

        down = dot(m_buf[...], v_wdown[...])
        h_buf[...] = (r_buf[...].astype(F32) + down + as_row(v_bdown)).astype(BF16)
        for start in range(0, tokens, rows):
            here = pl.ds(start, rows)
            z_buf[here, :] = layer_norm(h_buf[here, :].astype(F32), as_row(v_lnf_g), as_row(v_lnf_c)).astype(BF16)

        h_t[...] = z_buf[...].T

        for part in range(4):
            here = pl.ds(part * (DIM // 2), DIM // 2)
            kv_t[here, :] = add_column(dot(v_pwkv[here, :], h_t[...]), col_kv[here, :]).astype(BF16)

        @pl.when(s < local - 2)
        def _():
            for k in order:
                send(s + 2, k).start()

        scores = dot(u_diag[...], kv_t[pl.ds(0, DIM), :])
        top = jnp.max(scores, axis=1, keepdims=True)
        weights = jnp.exp2((scores - top) * (LOG2E * HEAD**-0.5))
        total = jnp.sum(weights, axis=1, keepdims=True)
        value = dot_nt(weights.astype(BF16), kv_t[pl.ds(DIM, DIM), :]) / total
        head_of_lane = lax.broadcasted_iota(jnp.int32, (16, DIM), 1) // HEAD
        diagonal = head_of_lane == lax.broadcasted_iota(jnp.int32, (16, DIM), 0)
        pooled = jnp.sum(jnp.where(diagonal, value, 0.0), axis=0, keepdims=True)
        a_buf[...] = jnp.where(lax.broadcasted_iota(jnp.int32, (8, DIM), 0) == s, pooled, a_buf[...])

        return 0

    lax.fori_loop(0, local, one_image, 0)

    pooled = a_buf[...].astype(BF16)
    o = (dot(pooled, v_pwout[...]) + as_row(v_pbout)).astype(BF16)
    normed = layer_norm(o.astype(F32), as_row(v_plng), as_row(v_plnc)).astype(BF16)
    hidden = gelu(dot(normed, v_pwup[...]) + as_row(v_pbup)).astype(BF16)
    emb[...] = (o.astype(F32) + dot(hidden, v_pwdown[...]) + as_row(v_pbdown))[:local, :]

    def share(k):
        return pltpu.make_async_remote_copy(
            src_ref=emb,
            dst_ref=out_ref.at[me],
            send_sem=emb_send.at[k],
            recv_sem=emb_recv.at[k],
            device_id={"cp": me ^ k},
            device_id_type=MESH,
        )

    for k in order:
        share(k).start()
    out_ref[me] = emb[...]
    for k in order:
        if k not in far:
            send(0, k).wait_send()
    for s in range(1, local):
        for k in order:
            send(s, k).wait_send()
    for k in order:
        share(k).wait()


def solution(mesh):
    group = mesh.shape["cp"]

    def device_step(
        images, ln1_scale, ln1_bias, w_qkv, b_qkv, w_out, b_out, ln2_scale, ln2_bias, w_up, b_up, w_down, b_down, lnf_scale, lnf_bias,
        pool_probe, pool_wq, pool_bq, pool_wkv, pool_bkv, pool_wout, pool_bout, pool_ln_scale, pool_ln_bias, pool_w_up, pool_b_up,
        pool_w_down, pool_b_down,
    ):
        count, run, _ = images.shape
        local = count // group
        tokens = group * run

        operands = [
            images, ln1_scale, ln1_bias, w_qkv.transpose(1, 2, 3, 0).reshape(3 * DIM, DIM), b_qkv,
            w_out.reshape(DIM, DIM), b_out, ln2_scale, ln2_bias, w_up, b_up, w_down, b_down,
            lnf_scale, lnf_bias, pool_probe, pool_wq.transpose(1, 2, 0).reshape(DIM, DIM), pool_bq,
            pool_wkv.transpose(1, 2, 3, 0).reshape(2 * DIM, DIM), pool_bkv.transpose(1, 0, 2), pool_wout.reshape(DIM, DIM),
            pool_bout, pool_ln_scale, pool_ln_bias, pool_w_up, pool_b_up, pool_w_down, pool_b_down,
        ]
        held = [pltpu.VMEM(operand.shape, operand.dtype) for operand in operands[1:]]
        scratch = [
            pltpu.VMEM((local, group, run, DIM), BF16),
            *held,
            pltpu.VMEM((DIM, DIM), BF16),
            pltpu.VMEM((3 * DIM, 128), F32),
            pltpu.VMEM((DIM, 128), F32),
            pltpu.VMEM((2 * DIM, 128), F32),
            pltpu.VMEM((1, DIM), F32),
            pltpu.VMEM((16, DIM), BF16),
            pltpu.VMEM((tokens, DIM), BF16),
            pltpu.VMEM((DIM, tokens), BF16),
            pltpu.VMEM((DIM, tokens), BF16),
            pltpu.VMEM((DIM, tokens), BF16),
            pltpu.VMEM((tokens, DIM), BF16),
            pltpu.VMEM((DIM, tokens), BF16),
            pltpu.VMEM((tokens, DIM), BF16),
            pltpu.VMEM((tokens, DIM), BF16),
            pltpu.VMEM((tokens, MLP), BF16),
            pltpu.VMEM((tokens, DIM), BF16),
            pltpu.VMEM((2 * DIM, tokens), BF16),
            pltpu.VMEM((2, tokens, 2 * tokens), F32),
            pltpu.VMEM((2, tokens, 2 * tokens), BF16),
            pltpu.VMEM((2, 1, 2 * tokens), F32),
            pltpu.VMEM((8, DIM), F32),
            pltpu.VMEM((local, DIM), F32),
            pltpu.SemaphoreType.DMA((len(held),)),
            pltpu.SemaphoreType.DMA((local,)),
            pltpu.SemaphoreType.DMA((local, group)),
            pltpu.SemaphoreType.DMA((local, group)),
            pltpu.SemaphoreType.DMA((group,)),
            pltpu.SemaphoreType.DMA((group,)),
            pltpu.SemaphoreType.REGULAR((2,)),
        ]
        result = pl.pallas_call(
            functools.partial(kernel, group, local, run),
            out_shape=jax.ShapeDtypeStruct((group, local, DIM), F32),
            in_specs=[pl.BlockSpec(memory_space=pl.ANY)] * len(operands),
            out_specs=pl.BlockSpec(memory_space=pltpu.VMEM),
            scratch_shapes=scratch,
            compiler_params=pltpu.CompilerParams(collective_id=0, has_side_effects=True, vmem_limit_bytes=67_043_328),
        )(*operands)
        return result.reshape(count, DIM)

    in_specs = (P("dp", "cp", None),) + (P(),) * 27
    return jax.shard_map(device_step, mesh=mesh, in_specs=in_specs, out_specs=P("dp", None), check_vma=False)
```

```python
import functools
import math

import jax
import jax.numpy as jnp
from jax import lax
from jax.experimental import pallas as pl
from jax.experimental.pallas import tpu as pltpu
from jax.sharding import PartitionSpec as P

MESH = pl.DeviceIdType.MESH
F32 = jnp.float32
BF16 = jnp.bfloat16
EPSILON = 1e-6
DIM = 768
HEADS = 12
HEAD = 64
MLP = 3072
GELU_C = math.sqrt(2.0 / math.pi)
LOG2E = math.log2(math.e)


def dot(left, right):
    return jnp.dot(left, right, preferred_element_type=F32)


def dot_nt(left, right):
    return lax.dot_general(left, right, (((1,), (1,)), ((), ())), preferred_element_type=F32)


def as_row(ref, cols=slice(None)):
    return ref[cols][None, :]


def gelu(x):
    half = 0.5 * x
    return half + half * jnp.tanh(x * (GELU_C + (GELU_C * 0.044715) * (x * x)))


def layer_norm(values, gain, shift):
    row_mean = jnp.sum(values, axis=-1, keepdims=True) * (1.0 / DIM)
    centered = values - row_mean
    variance = jnp.sum(centered * centered, axis=-1, keepdims=True) * (1.0 / DIM)
    return centered * lax.rsqrt(variance + EPSILON) * gain + shift


def column_bias(bias, out_ref, base):
    eye = lax.broadcasted_iota(jnp.int32, (HEAD, HEAD), 0) == lax.broadcasted_iota(jnp.int32, (HEAD, HEAD), 1)
    for head in range(HEADS):
        spread = jnp.where(eye, jnp.broadcast_to(bias[head : head + 1, :], (HEAD, HEAD)), 0.0)
        column = jnp.sum(spread, axis=1, keepdims=True)
        out_ref[pl.ds(base + head * HEAD, HEAD), :] = jnp.broadcast_to(column, (HEAD, 128))


def row_bias(column_ref, base):
    eye = lax.broadcasted_iota(jnp.int32, (128, 128), 0) == lax.broadcasted_iota(jnp.int32, (128, 128), 1)
    parts = []
    for block in range(DIM // 128):
        tile = column_ref[pl.ds(base + block * 128, 128), :]
        parts.append(jnp.sum(jnp.where(eye, tile, 0.0), axis=0, keepdims=True))
    return jnp.concatenate(parts, axis=1)


def add_column(values, column):
    return values + jnp.concatenate([column, column], axis=1)


def kernel(
    group, local, run,
    images, ln1_g, ln1_c, w_qkv, b_qkv, w_out, b_out, ln2_g, ln2_c, w_up, b_up, w_down, b_down, lnf_g, lnf_c,
    probe, p_wq, p_bq, p_wkv, p_bkv, p_wout, p_bout, pln_g, pln_c, p_wup, p_bup, p_wdown, p_bdown,
    out_ref,
    x_buf, v_ln1_g, v_ln1_c, v_wqkv, v_bqkv, v_wout, v_bout, v_ln2_g, v_ln2_c, v_wup, v_bup, v_wdown, v_bdown, v_lnf_g, v_lnf_c,
    v_probe, v_pwq, v_pbq, v_pwkv, v_pbkv, v_pwout, v_pbout, v_plng, v_plnc, v_pwup, v_pbup, v_pwdown, v_pbdown,
    wk_t, col_qkv, col_q, col_kv, row_k, u_diag, h_buf, h_t, q_t, v_t, k_buf, c_t, r_buf, n_buf, m_buf, z_buf, kv_t, s_buf, w_buf, t_buf, a_buf, emb,
    load_sem, own_sem, send_sem, recv_sem, emb_send, emb_recv, relay,
):
    tokens = group * run
    me = lax.axis_index("cp")
    chip = me // 2
    inner = (chip == 1) | (chip == 2)

    def tell(semaphore, k):
        pl.semaphore_signal(semaphore, inc=1, device_id={"cp": me ^ k}, device_id_type=MESH)

    barrier = pltpu.get_barrier_semaphore()
    for k in (2, 3, 1):
        tell(barrier, k)

    @pl.when(inner)
    def _():
        tell(barrier, 6)
        tell(barrier, 7)

    pairs = [
        (w_qkv, v_wqkv), (ln1_g, v_ln1_g), (ln1_c, v_ln1_c), (b_qkv, v_bqkv), (w_out, v_wout), (b_out, v_bout),
        (ln2_g, v_ln2_g), (ln2_c, v_ln2_c), (w_up, v_wup), (b_up, v_bup), (w_down, v_wdown), (b_down, v_bdown),
        (lnf_g, v_lnf_g), (lnf_c, v_lnf_c), (probe, v_probe), (p_wq, v_pwq), (p_bq, v_pbq), (p_wkv, v_pwkv),
        (p_bkv, v_pbkv), (p_wout, v_pwout), (p_bout, v_pbout), (pln_g, v_plng), (pln_c, v_plnc), (p_wup, v_pwup),
        (p_bup, v_pbup), (p_wdown, v_pwdown), (p_bdown, v_pbdown),
    ]
    loads = [pltpu.make_async_copy(src, dst, load_sem.at[i]) for i, (src, dst) in enumerate(pairs)]
    own = [pltpu.make_async_copy(images.at[me * local + s], x_buf.at[s, me], own_sem.at[s]) for s in range(local)]
    for copy in loads[:4]:
        copy.start()
    for copy in own:
        copy.start()

    def send(s, k):
        peer = me ^ k
        return pltpu.make_async_remote_copy(
            src_ref=images.at[peer * local + s],
            dst_ref=x_buf.at[s, me],
            send_sem=send_sem.at[s, k],
            recv_sem=recv_sem.at[s, k],
            device_id={"cp": peer},
            device_id_type=MESH,
        )

    far, near = (6, 7, 4, 5), (2, 3, 1)
    order = far + near

    @pl.when(inner)
    def _():
        pl.semaphore_wait(barrier, 5)
        send(0, 6).start()
        send(0, 7).start()
        tell(relay.at[0], 2)
        tell(relay.at[0], 6)

    @pl.when(jnp.logical_not(inner))
    def _():
        pl.semaphore_wait(barrier, 3)

    for k in near:
        send(0, k).start()
    for copy in loads[4:]:
        copy.start()
    pl.semaphore_wait(relay.at[0], 1)

    @pl.when(inner)
    def _():
        tell(relay.at[1], 2)

    send(0, 4).start()
    send(0, 5).start()

    @pl.when(jnp.logical_not(inner))
    def _():
        pl.semaphore_wait(relay.at[1], 1)
        send(0, 6).start()
        send(0, 7).start()

    for copy in loads[:4]:
        copy.wait()

    for part in range(3):
        column_bias(v_bqkv[part], col_qkv, part * DIM)
    row_k[...] = row_bias(col_qkv, DIM)
    for block in range(DIM // 256):
        wk_t[:, pl.ds(block * 256, 256)] = v_wqkv[pl.ds(DIM + block * 256, 256), :].T
    for copy in loads[4:]:
        copy.wait()
    column_bias(v_pbq[...], col_q, 0)
    column_bias(v_pbkv[:, 0, :], col_kv, 0)
    column_bias(v_pbkv[:, 1, :], col_kv, DIM)
    @pl.when(jnp.logical_not(inner))
    def _():
        for k in order:
            send(1, k).start()

    probe_rows = jnp.broadcast_to(v_probe[...].astype(F32), (16, DIM)).astype(BF16)
    probe_q = dot_nt(probe_rows, v_pwq[...]) + row_bias(col_q, 0)
    head_of_lane = lax.broadcasted_iota(jnp.int32, (16, DIM), 1) // HEAD
    diagonal = head_of_lane == lax.broadcasted_iota(jnp.int32, (16, DIM), 0)
    u_diag[...] = jnp.where(diagonal, probe_q, 0.0).astype(BF16)

    rows = 32
    a_buf[...] = jnp.zeros_like(a_buf)

    @pl.when(inner)
    def _():
        for k in far:
            send(0, k).wait_send()
        for k in order:
            send(1, k).start()


    def one_image(s, _):
        pltpu.make_async_copy(images.at[0], x_buf.at[s, me], own_sem.at[s]).wait()
        for ks in (near + (0,), far):
            for k in ks:
                if k:
                    send(s, k).wait_recv()
            for k in ks:
                here = pl.ds(pl.multiple_of((me ^ k) * run, run), run)
                x = x_buf[s, me ^ k].astype(F32)
                h_buf[here, :] = layer_norm(x, as_row(v_ln1_g), as_row(v_ln1_c)).astype(BF16)

        h_t[...] = h_buf[...].T

        q_t[...] = add_column(dot(v_wqkv[pl.ds(0, DIM), :], h_t[...]), col_qkv[pl.ds(0, DIM), :]).astype(BF16)
        v_t[...] = add_column(dot(v_wqkv[pl.ds(2 * DIM, DIM), :], h_t[...]), col_qkv[pl.ds(2 * DIM, DIM), :]).astype(BF16)
        k_buf[...] = (dot(h_buf[...], wk_t[...]) + row_k[...]).astype(BF16)

        pairs = HEADS // 2
        zero = jnp.zeros((HEAD, tokens), BF16)
        for step in range(pairs + 2):
            if step < pairs:
                k_pair = k_buf[:, pl.ds(step * 2 * HEAD, 2 * HEAD)]
                low = q_t[pl.ds(2 * step * HEAD, HEAD), :]
                high = q_t[pl.ds((2 * step + 1) * HEAD, HEAD), :]
                s_buf[step % 2, :, pl.ds(0, tokens)] = dot(k_pair, jnp.concatenate([low, zero], axis=0))
                s_buf[step % 2, :, pl.ds(tokens, tokens)] = dot(k_pair, jnp.concatenate([zero, high], axis=0))
            if 1 <= step <= pairs:
                slot = (step - 1) % 2
                for block in range(2 * tokens // 128):
                    cols = pl.ds(block * 128, 128)
                    top = jnp.max(s_buf[slot, :, cols], axis=0, keepdims=True)
                    weights = jnp.exp2((s_buf[slot, :, cols] - top) * (LOG2E * HEAD**-0.5))
                    t_buf[slot, :, cols] = 1.0 / jnp.sum(weights, axis=0, keepdims=True)
                    w_buf[slot, :, cols] = weights.astype(BF16)
            if step >= 2:
                slot = step % 2
                for side in range(2):
                    here = pl.ds((2 * (step - 2) + side) * HEAD, HEAD)
                    cols = pl.ds(side * tokens, tokens)
                    c_t[here, :] = (dot(v_t[here, :], w_buf[slot, :, cols]) * t_buf[slot, :, cols]).astype(BF16)

        h_buf[...] = c_t[...].T

        half_rows = tokens // 2
        for half in range(2):
            here = pl.ds(half * half_rows, half_rows)
            attn = dot(h_buf[here, :], v_wout[...]) + as_row(v_bout)
            for part in range(group // 2):
                piece = half * (group // 2) + part
                r_buf[pl.ds(piece * run, run), :] = (x_buf[s, piece].astype(F32) + attn[part * run : (part + 1) * run, :]).astype(BF16)
            for start in range(0, half_rows, rows):
                some = pl.ds(half * half_rows + start, rows)
                n_buf[some, :] = layer_norm(r_buf[some, :].astype(F32), as_row(v_ln2_g), as_row(v_ln2_c)).astype(BF16)
        for half in range(2):
            here = pl.ds(half * half_rows, half_rows)
            for block in range(MLP // 512):
                cols = pl.ds(block * 512, 512)
                m_buf[here, cols] = gelu(dot(n_buf[here, :], v_wup[:, cols]) + as_row(v_bup, cols)).astype(BF16)
        for half in range(2):
            here = pl.ds(half * half_rows, half_rows)
            down = dot(m_buf[here, :], v_wdown[...])
            h_buf[here, :] = (r_buf[here, :].astype(F32) + down + as_row(v_bdown)).astype(BF16)
            for start in range(0, half_rows, rows):
                some = pl.ds(half * half_rows + start, rows)
                z_buf[some, :] = layer_norm(h_buf[some, :].astype(F32), as_row(v_lnf_g), as_row(v_lnf_c)).astype(BF16)
        h_t[...] = z_buf[...].T

        for part in range(2):
            here = pl.ds(part * (DIM // 2), DIM // 2)
            kv_t[here, :] = add_column(dot(v_pwkv[here, :], h_t[...]), col_kv[here, :]).astype(BF16)
        scores = dot(u_diag[...], kv_t[pl.ds(0, DIM), :])
        for part in range(2, 4):
            here = pl.ds(part * (DIM // 2), DIM // 2)
            kv_t[here, :] = add_column(dot(v_pwkv[here, :], h_t[...]), col_kv[here, :]).astype(BF16)
        top = jnp.max(scores, axis=1, keepdims=True)
        weights = jnp.exp2((scores - top) * (LOG2E * HEAD**-0.5))
        total = jnp.sum(weights, axis=1, keepdims=True)
        value = dot_nt(weights.astype(BF16), kv_t[pl.ds(DIM, DIM), :]) / total
        head_of_lane = lax.broadcasted_iota(jnp.int32, (16, DIM), 1) // HEAD
        diagonal = head_of_lane == lax.broadcasted_iota(jnp.int32, (16, DIM), 0)
        pooled = jnp.sum(jnp.where(diagonal, value, 0.0), axis=0, keepdims=True)
        a_buf[...] = jnp.where(lax.broadcasted_iota(jnp.int32, (8, DIM), 0) == s, pooled, a_buf[...])

        @pl.when(s < local - 2)
        def _():
            for k in order:
                send(s + 2, k).start()

        return 0

    lax.fori_loop(0, local, one_image, 0)

    pooled = a_buf[...].astype(BF16)
    o = (dot(pooled, v_pwout[...]) + as_row(v_pbout)).astype(BF16)
    normed = layer_norm(o.astype(F32), as_row(v_plng), as_row(v_plnc)).astype(BF16)
    hidden = gelu(dot(normed, v_pwup[...]) + as_row(v_pbup)).astype(BF16)
    emb[...] = (o.astype(F32) + dot(hidden, v_pwdown[...]) + as_row(v_pbdown))[:local, :]

    def share(k):
        return pltpu.make_async_remote_copy(
            src_ref=emb,
            dst_ref=out_ref.at[pl.ds(pl.multiple_of(me * local, local), local)],
            send_sem=emb_send.at[k],
            recv_sem=emb_recv.at[k],
            device_id={"cp": me ^ k},
            device_id_type=MESH,
        )

    for k in order:
        share(k).start()
    mine = pltpu.make_async_copy(emb, out_ref.at[pl.ds(pl.multiple_of(me * local, local), local)], emb_send.at[0])
    mine.start()
    mine.wait()
    for k in near:
        send(0, k).wait_send()

    @pl.when(jnp.logical_not(inner))
    def _():
        for k in far:
            send(0, k).wait_send()

    for s in range(1, local):
        for k in order:
            send(s, k).wait_send()
    for k in order:
        share(k).wait()


def solution(mesh):
    group = mesh.shape["cp"]

    def device_step(
        images, ln1_scale, ln1_bias, w_qkv, b_qkv, w_out, b_out, ln2_scale, ln2_bias, w_up, b_up, w_down, b_down, lnf_scale, lnf_bias,
        pool_probe, pool_wq, pool_bq, pool_wkv, pool_bkv, pool_wout, pool_bout, pool_ln_scale, pool_ln_bias, pool_w_up, pool_b_up,
        pool_w_down, pool_b_down,
    ):
        count, run, _ = images.shape
        local = count // group
        tokens = group * run

        operands = [
            images, ln1_scale, ln1_bias, w_qkv.transpose(1, 2, 3, 0).reshape(3 * DIM, DIM), b_qkv,
            w_out.reshape(DIM, DIM), b_out, ln2_scale, ln2_bias, w_up, b_up, w_down, b_down,
            lnf_scale, lnf_bias, pool_probe, pool_wq.transpose(1, 2, 0).reshape(DIM, DIM), pool_bq,
            pool_wkv.transpose(1, 2, 3, 0).reshape(2 * DIM, DIM), pool_bkv.transpose(1, 0, 2), pool_wout.reshape(DIM, DIM),
            pool_bout, pool_ln_scale, pool_ln_bias, pool_w_up, pool_b_up, pool_w_down, pool_b_down,
        ]
        held = [pltpu.VMEM(operand.shape, operand.dtype) for operand in operands[1:]]
        scratch = [
            pltpu.VMEM((local, group, run, DIM), BF16),
            *held,
            pltpu.VMEM((DIM, DIM), BF16),
            pltpu.VMEM((3 * DIM, 128), F32),
            pltpu.VMEM((DIM, 128), F32),
            pltpu.VMEM((2 * DIM, 128), F32),
            pltpu.VMEM((1, DIM), F32),
            pltpu.VMEM((16, DIM), BF16),
            pltpu.VMEM((tokens, DIM), BF16),
            pltpu.VMEM((DIM, tokens), BF16),
            pltpu.VMEM((DIM, tokens), BF16),
            pltpu.VMEM((DIM, tokens), BF16),
            pltpu.VMEM((tokens, DIM), BF16),
            pltpu.VMEM((DIM, tokens), BF16),
            pltpu.VMEM((tokens, DIM), BF16),
            pltpu.VMEM((tokens, DIM), BF16),
            pltpu.VMEM((tokens, MLP), BF16),
            pltpu.VMEM((tokens, DIM), BF16),
            pltpu.VMEM((2 * DIM, tokens), BF16),
            pltpu.VMEM((2, tokens, 2 * tokens), F32),
            pltpu.VMEM((2, tokens, 2 * tokens), BF16),
            pltpu.VMEM((2, 1, 2 * tokens), F32),
            pltpu.VMEM((8, DIM), F32),
            pltpu.VMEM((local, DIM), F32),
            pltpu.SemaphoreType.DMA((len(held),)),
            pltpu.SemaphoreType.DMA((local,)),
            pltpu.SemaphoreType.DMA((local, group)),
            pltpu.SemaphoreType.DMA((local, group)),
            pltpu.SemaphoreType.DMA((group,)),
            pltpu.SemaphoreType.DMA((group,)),
            pltpu.SemaphoreType.REGULAR((2,)),
        ]
        result = pl.pallas_call(
            functools.partial(kernel, group, local, run),
            out_shape=jax.ShapeDtypeStruct((count, DIM), F32),
            in_specs=[pl.BlockSpec(memory_space=pl.ANY)] * len(operands),
            out_specs=pl.BlockSpec(memory_space=pl.ANY),
            scratch_shapes=scratch,
            compiler_params=pltpu.CompilerParams(collective_id=0, has_side_effects=True, vmem_limit_bytes=67_043_328),
        )(*operands)
        return result

    in_specs = (P("dp", "cp", None),) + (P(),) * 27
    return jax.shard_map(device_step, mesh=mesh, in_specs=in_specs, out_specs=P("dp", None), check_vma=False)
```
